32 devices in a mesh: dp: 16 (over z, y, core), tensor: 2 (over x).
Axes of the slice: x: 2, y: 2, z: 4, core: 2. Of those that a mesh axis runs over, the one named last changes fastest.
Arguments:
- tokens: bfloat16 [16384, 1024], P('dp'), may hold values from -6 to 6
- cotangent: bfloat16 [16384, 1024], P('dp'), may hold values from -6 to 6
- attn_gain: float32 [1024], replicated, may hold values from 0.1 to 1.9
- mlp_gain: float32 [1024], replicated, may hold values from 0.1 to 1.9
- w_qkv: bfloat16 [1024, 3, 1024], P(None, None, 'tensor'), may hold values from -0.1875 to 0.1875
- w_out: bfloat16 [1024, 1024], P('tensor'), may hold values from -0.75 to 0.75
- w_in: bfloat16 [1024, 2, 2624], P(None, None, 'tensor'), may hold values from -0.1875 to 0.1875
- w_down: bfloat16 [2624, 1024], P('tensor'), may hold values from -0.125 to 0.125
- seq_lengths: int32 [16, 4], replicated, may hold values from 1 to 512, as said below
- set_owner: int32 [16], replicated, may hold values from 0 to 15, each once
- arrival: int32 [1024], replicated, may hold values from 0 to 1023, as said below
Outputs:
- output: float32 [16384, 1024], P('dp')
- grad_tokens: float32 [16384, 1024], P('dp')
- grad_attn_gain: float32 [1024], P('dp')
- grad_mlp_gain: float32 [1024], P('dp')
- grad_qkv: float32 [1024, 3, 1024], P('dp', None, 'tensor')
- grad_out: float32 [1024, 1024], P('tensor', 'dp')
- grad_in: float32 [1024, 2, 2624], P('dp', None, 'tensor')
- grad_down: float32 [2624, 1024], P('tensor', 'dp')
The draws below stay inside these ranges and needn't reach their ends.
Inputs may be any that keep to these rules, and one draw needn't show every extreme that they name: `seq_lengths`: each row holds the lengths of the 4 sequences of one set; they sum to 1024, and exactly one of them is 512. Set b is taken by data group set_owner[b]; each group takes one set. `arrival`: A permutation of the group layout's pieces; piece p belongs to group p // 64. The 64 pieces that stand on one data index go to 16 groups, exactly 4 to each.
All inputs are finite; a program needn't handle non-finite values.
Results may differ from the reference program's by a relative error of at most 0.017.
The reference program's roundings to bfloat16 on the way count: a program that leaves them out, or rounds other values in their place, can miss the bound.
Values may be sent and summed in bfloat16 or wider, within the bound.
A program may use at most 256 MiB of HBM per device.

```python
import jax
import jax.numpy as jnp
from jax import lax

D = 1024
HEADS = 16
HEAD = 64
FF = 2624
TOK_DEV = 1024
NSEQ = 4
QBLOCK = 512
PIECES = 64
PAIR = 4
LONGEST = 512
TOKENS = 16384
N_DP = 16


def draw_seq_lengths(key, part):

    def one_set(set_key):
        first_key, second_key = jax.random.split(set_key)
        remain = TOK_DEV - LONGEST
        cuts = jnp.sort(jax.random.permutation(first_key, remain - 1)[:NSEQ - 2].astype(jnp.int32) + 1)
        edges = jnp.concatenate([jnp.zeros((1,), jnp.int32), cuts, jnp.full((1,), remain, jnp.int32)])
        others = edges[1:] - edges[:-1]
        values = jnp.concatenate([jnp.full((1,), LONGEST, jnp.int32), others])
        return values[jax.random.permutation(second_key, NSEQ)]
    return jax.vmap(one_set)(jax.random.split(key, N_DP)).astype(jnp.int32)


def draw_arrival(key, part):
    key_one, key_two, key_three, key_four = jax.random.split(key, 4)
    spread = PIECES // PAIR
    shifted = jax.random.permutation(key_one, N_DP).astype(jnp.int32)
    offsets = jax.random.permutation(key_two, N_DP)[:spread].astype(jnp.int32)
    slot_order = jax.vmap(lambda sub: jax.random.permutation(sub, PIECES))(jax.random.split(key_three, N_DP)).astype(jnp.int32)
    target_group = (shifted[:, None] + offsets[slot_order // PAIR]) % N_DP
    within = jax.vmap(lambda sub: jax.random.permutation(sub, PIECES))(jax.random.split(key_four, N_DP)).astype(jnp.int32)
    chosen = within[target_group, slot_order]
    return (target_group * PIECES + chosen).reshape(-1).astype(jnp.int32)


def shard_levels(own_key, dims, cuts, least, largest):
    factor_of = 1.0
    for dim, shards_of in cuts:
        heights = jax.random.uniform(jax.random.fold_in(jax.random.fold_in(own_key, 6), dim), (shards_of,), jnp.float32, least / len(cuts), largest / len(cuts))
        factor_of = factor_of * jnp.repeat(jnp.exp(heights), dims[dim] // shards_of).reshape((-1,) + (1,) * (len(dims) - 1 - dim))
    return factor_of


def noise(rng, extent, deviation, bound, cuts=(), kind=jnp.bfloat16):
    entries = jax.random.normal(rng, extent, jnp.float32) * deviation
    if len(cuts) > 0:
        entries = shard_levels(rng, extent, cuts, -0.22, 0.18) * entries
    return jnp.clip(entries, min=-bound, max=bound).astype(kind)


def setup_inputs(seed: int = 0) -> dict:
    keys = jax.random.split(jax.random.key(seed), 12)
    return {
        "tokens": noise(keys[0], (TOKENS, D), 1.0, 6.0, ((0, 16),)),
        "cotangent": noise(keys[1], (TOKENS, D), 1.0, 6.0, ((0, 16),)),
        "attn_gain": jnp.clip(1.0 + 0.18 * jax.random.normal(keys[2], (D,), jnp.float32), 0.1, 1.9),
        "mlp_gain": jnp.clip(1.0 + 0.18 * jax.random.normal(keys[3], (D,), jnp.float32), 0.1, 1.9),
        "w_qkv": noise(keys[4], (D, 3, D), D ** -0.5, 0.1875, ((2, 2),)),
        "w_out": noise(keys[5], (D, D), (D // 16) ** -0.5, 0.75, ((0, 2),)),
        "w_in": noise(keys[6], (D, 2, FF), D ** -0.5, 0.1875, ((2, 2),)),
        "w_down": noise(keys[7], (FF, D), FF ** -0.5, 0.125, ((0, 2),)),
        "seq_lengths": draw_seq_lengths(jax.random.fold_in(keys[11], 71), 0),
        "set_owner": jax.random.permutation(keys[9], N_DP).astype(jnp.int32),
        "arrival": draw_arrival(jax.random.fold_in(keys[11], 71), 0),
    }


@jax.custom_vjp
def low(v):
    return lax.optimization_barrier(v.astype(jnp.bfloat16)).astype(jnp.float32)

@jax.custom_vjp
def low_back(v):
    return v

def low_keep(v):
    return (low(v), None)

def low_pass(kept, grad):
    return (grad,)

def back_keep(v):
    return (v, None)

def back_low(kept, grad):
    return (low(grad),)
low.defvjp(low_keep, low_pass)
low_back.defvjp(back_keep, back_low)
EPSILON = 1e-05
THETA_BASE = 160000.0
SCORE_SCALE = 0.125
MASK_FILL = -1000000000.0
HIGHEST = lax.Precision.HIGHEST

def norm_rows(values, gain):
    centred = values - lax.optimization_barrier(jnp.mean(values, axis=-1, keepdims=True))
    return centred * lax.rsqrt(lax.optimization_barrier(jnp.mean(centred * centred, axis=-1, keepdims=True)) + EPSILON) * gain

def rotary(position):
    halves = HEAD // 2
    frequency = THETA_BASE ** (-2.0 * jnp.arange(halves, dtype=jnp.float32) / HEAD)
    angles = position.astype(jnp.float32)[:, None] * frequency[None, :]
    cosine = jnp.concatenate([jnp.cos(angles), jnp.cos(angles)], axis=-1)[:, None, :]
    sine = jnp.concatenate([jnp.sin(angles), jnp.sin(angles)], axis=-1)[:, None, :]
    return (cosine, sine)

def spin(values, cosine, sine):
    halves = values.shape[-1] // 2
    turned = jnp.concatenate([-values[..., halves:], values[..., :halves]], axis=-1)
    return values * cosine + turned * sine

def segments(lengths_row, row_count):
    ends = jnp.cumsum(lengths_row).astype(jnp.int32)
    rows = jnp.arange(row_count, dtype=jnp.int32)
    segment = lax.optimization_barrier(jnp.sum((rows[:, None] >= ends[None, :]).astype(jnp.int32), axis=1)).astype(jnp.int32)
    starts = (ends - lengths_row).astype(jnp.int32)
    matches = segment[:, None] == jnp.arange(lengths_row.shape[0], dtype=jnp.int32)[None, :]
    first_rows = lax.optimization_barrier(jnp.sum(jnp.where(matches, starts[None, :], 0), axis=1)).astype(jnp.int32)
    return (segment, (rows - first_rows).astype(jnp.int32))

def attention(queries, key_rows, value_rows, segment, row_count):

    def one_block(first_row):
        block = lax.dynamic_slice_in_dim(queries, first_row, QBLOCK, 0)
        block_seg = lax.dynamic_slice_in_dim(segment, first_row, QBLOCK, 0)
        scores = low_back(jnp.einsum('qhe,khe->hqk', block, key_rows, precision=HIGHEST) * SCORE_SCALE)
        allowed = (block_seg[:, None] == segment[None, :])[None]
        probs = low(jax.nn.softmax(jnp.where(allowed, scores, MASK_FILL), axis=-1))
        return jnp.einsum('hqk,khe->qhe', probs, value_rows, precision=HIGHEST)
    starts = (jnp.arange(row_count // QBLOCK, dtype=jnp.int32) * QBLOCK).astype(jnp.int32)
    blocks = lax.map(jax.checkpoint(one_block), starts)
    return blocks.reshape(row_count, D)

def forward(inputs_x, weights, segment, position):
    attn_gain, mlp_gain, w_qkv, w_out, w_in, w_down = weights
    row_count = inputs_x.shape[0]
    normed = low(norm_rows(inputs_x, attn_gain))
    mixed = low_back(jnp.einsum('td,dcf->tcf', normed, w_qkv, precision=HIGHEST))
    heads_view = mixed.reshape(row_count, 3, HEADS, HEAD)
    cosine, sine = rotary(position)
    queries = low(spin(heads_view[:, 0], cosine, sine))
    key_rows = low(spin(heads_view[:, 1], cosine, sine))
    value_rows = low(heads_view[:, 2])
    attended = low_back(low(attention(queries, key_rows, value_rows, segment, row_count)))
    branch = low_back(jnp.dot(attended, w_out, precision=HIGHEST))
    hidden = inputs_x + branch
    normed_two = low(norm_rows(hidden, mlp_gain))
    gate_up = low_back(jnp.einsum('td,dcf->tcf', normed_two, w_in, precision=HIGHEST))
    product = low(jax.nn.gelu(gate_up[:, 0], approximate=False) * gate_up[:, 1])
    return hidden + jnp.dot(product, w_down, precision=HIGHEST)

def reference(tokens, cotangent, attn_gain, mlp_gain, w_qkv, w_out, w_in, w_down, seq_lengths, set_owner, arrival):
    piece_total = arrival.shape[0]
    group_total = set_owner.shape[0]
    row_count = tokens.shape[0] // group_total
    piece_rows = tokens.shape[0] // piece_total
    model_width = tokens.shape[1]

    def arrange(values):
        shaped = values.astype(jnp.float32).reshape(piece_total, piece_rows, model_width)
        return jnp.zeros_like(shaped).at[arrival].set(shaped).reshape(group_total, row_count, model_width)
    lengths_held = jnp.zeros_like(seq_lengths).at[set_owner].set(seq_lengths)
    params = tuple((param.astype(jnp.float32) for param in (attn_gain, mlp_gain, w_qkv, w_out, w_in, w_down)))

    def one_group(carry, inputs):
        group_x, group_c, group_len = inputs
        segment, position = segments(group_len, row_count)

        def layer(inputs_x, *weights):
            return forward(inputs_x, weights, segment, position)
        result, pull = jax.vjp(layer, group_x, *params)
        grads = pull(group_c)
        return (tuple((acc + fresh for acc, fresh in zip(carry, grads[1:]))), (result, grads[0]))
    start = tuple((jnp.zeros_like(param) for param in params))
    sums, (results, input_grads) = lax.scan(one_group, start, (arrange(tokens), arrange(cotangent), lengths_held))

    def unarrange(values):
        return values.reshape(piece_total, piece_rows, model_width)[arrival].reshape(tokens.shape[0], model_width)
    return (unarrange(results), unarrange(input_grads), sums[0], sums[1], sums[2], sums[3], sums[4], sums[5])
```

```python
import jax
import jax.numpy as jnp
from jax import lax
from jax.sharding import PartitionSpec as P

HEAD = 64
EPSILON = 1e-05
THETA_BASE = 160000.0
SCORE_SCALE = 0.125
MASK_FILL = -1000000000.0
ROOT_HALF = 0.7071067811865476
ROOT_TWO_PI_INV = 0.3989422804014327


def low(values):
    return values.astype(jnp.bfloat16)


def wide(values):
    return values.astype(jnp.float32)


def norm_parts(values):
    centred = values - jnp.mean(values, axis=-1, keepdims=True)
    scale = lax.rsqrt(jnp.mean(centred * centred, axis=-1, keepdims=True) + EPSILON)
    return (centred * scale, scale)


def norm_back(unit, scale, grad):
    mean_grad = jnp.mean(grad, axis=-1, keepdims=True)
    mean_along = jnp.mean(grad * unit, axis=-1, keepdims=True)
    return scale * (grad - mean_grad - unit * mean_along)


def rotary(position):
    halves = HEAD // 2
    frequency = THETA_BASE ** (-2.0 * jnp.arange(halves, dtype=jnp.float32) / HEAD)
    angles = position.astype(jnp.float32)[:, None] * frequency[None, :]
    cosine = jnp.concatenate([jnp.cos(angles), jnp.cos(angles)], axis=-1)[:, None, :]
    sine = jnp.concatenate([jnp.sin(angles), jnp.sin(angles)], axis=-1)[:, None, :]
    return (cosine, sine)


def spin(values, cosine, sine):
    halves = values.shape[-1] // 2
    turned = jnp.concatenate([-values[..., halves:], values[..., :halves]], axis=-1)
    return values * cosine + turned * sine


def spin_back(grads, cosine, sine):
    halves = grads.shape[-1] // 2
    scaled = grads * sine
    turned = jnp.concatenate([scaled[..., halves:], -scaled[..., :halves]], axis=-1)
    return grads * cosine + turned


def segments(lengths_row, row_count):
    ends = jnp.cumsum(lengths_row)
    rows = jnp.arange(row_count, dtype=jnp.int32)
    segment = jnp.sum((rows[:, None] >= ends[None, :]).astype(jnp.int32), axis=1)
    starts = ends - lengths_row
    matches = segment[:, None] == jnp.arange(lengths_row.shape[0], dtype=jnp.int32)[None, :]
    first_rows = jnp.sum(jnp.where(matches, starts[None, :], 0), axis=1)
    long_start = jnp.sum(jnp.where(lengths_row * 2 == row_count, starts, 0))
    return (segment, rows - first_rows, long_start)


def swap_sum(part):
    mine = lax.optimization_barrier(low(part))
    other = lax.ppermute(mine, "tensor", [(0, 1), (1, 0)])
    return wide(mine) + wide(other)


def scatter_sum(grad, group_total, group_index):
    bits = group_total.bit_length() - 1
    rows = grad.shape[0] // group_total
    tail = grad.shape[1:]
    value = grad.reshape((2,) * bits + (rows,) + tail)
    for bit in range(bits):
        axis = bits - 1 - bit
        mine = (group_index >> bit) & 1
        send = lax.dynamic_index_in_dim(value, 1 - mine, axis, keepdims=False)
        keep = lax.dynamic_index_in_dim(value, mine, axis, keepdims=False)
        if value.dtype == jnp.float32 and grad.ndim > 1:
            send = low(send)
        pairs = [(device, device ^ (1 << bit)) for device in range(group_total)]
        got = lax.ppermute(send, "dp", pairs)
        value = wide(keep) + wide(got)
    return value


def scores_of(queries, keys, allowed):
    scores = (
        jnp.einsum("qhe,khe->hqk", queries, keys, preferred_element_type=jnp.float32) * SCORE_SCALE
    )
    if allowed is not None:
        scores = jnp.where(allowed, scores, MASK_FILL)
    return scores


def on_device(
    tokens,
    cotangent,
    attn_gain,
    mlp_gain,
    w_qkv,
    w_out,
    w_in,
    w_down,
    seq_lengths,
    set_owner,
    arrival,
):
    group_total = lax.axis_size("dp")
    group_index = lax.axis_index("dp")
    row_count = tokens.shape[0]
    model_width = tokens.shape[1]
    piece_count = arrival.shape[0] // group_total
    piece_rows = row_count // piece_count
    pair_cap = max(2, piece_count // group_total)
    slot_count = group_total * pair_cap
    target = arrival.reshape(group_total, piece_count)
    target_group = target // piece_count
    target_place = target % piece_count
    piece_ids = jnp.arange(piece_count, dtype=jnp.int32)
    earlier = piece_ids[None, :] < piece_ids[:, None]
    same_group = target_group[:, :, None] == target_group[:, None, :]
    slot_rank = jnp.sum((same_group & earlier[None]).astype(jnp.int32), axis=2)
    send_slot = target_group * pair_cap + slot_rank
    own_slots = lax.dynamic_index_in_dim(send_slot, group_index, 0, keepdims=False)
    slot_ids = jnp.arange(slot_count, dtype=jnp.int32)
    outgoing = own_slots[None, :] == slot_ids[:, None]
    out_piece = jnp.sum(jnp.where(outgoing, piece_ids[None, :], 0), axis=1)
    toward = target_group == group_index
    rank_ids = jnp.arange(pair_cap, dtype=jnp.int32)
    incoming = toward[:, None, :] & (slot_rank[:, None, :] == rank_ids[None, :, None])
    in_place = jnp.sum(jnp.where(incoming, target_place[:, None, :], 0), axis=2).reshape(slot_count)
    in_live = jnp.any(incoming, axis=2).reshape(slot_count)
    chosen = (in_place[None, :] == piece_ids[:, None]) & in_live[None, :]
    in_slot = jnp.sum(jnp.where(chosen, slot_ids[None, :], 0), axis=1)

    def take_pieces(values, ids, count):
        return (
            values.reshape(count, piece_rows, model_width)
            .at[ids]
            .get(mode="promise_in_bounds")
            .reshape(-1, model_width)
        )

    def deal(values):
        return lax.all_to_all(values, "dp", split_axis=0, concat_axis=0, tiled=True)

    held = set_owner == group_index
    lengths_mine = jnp.sum(jnp.where(held[:, None], seq_lengths, 0), axis=0)
    segment, position, long_start = segments(lengths_mine, row_count)
    half = row_count // 2
    low_first = jnp.arange(half, dtype=jnp.int32) < long_start

    def split(values):
        mask = low_first.reshape((half,) + (1,) * (values.ndim - 1))
        first, second = (values[:half], values[half:])
        return (jnp.where(mask, first, second), jnp.where(mask, second, first))

    def join(rest, long):
        mask = low_first.reshape((half,) + (1,) * (rest.ndim - 1))
        return jnp.concatenate([jnp.where(mask, rest, long), jnp.where(mask, long, rest)], axis=0)

    tokens_in = deal(take_pieces(tokens, out_piece, piece_count))
    inputs_pair = split(take_pieces(tokens_in, in_slot, slot_count))
    grads_in = deal(take_pieces(cotangent, out_piece, piece_count))
    grads_pair = split(take_pieces(grads_in, in_slot, slot_count))
    position_pair = split(position)
    seg_rest, _ = split(segment)
    allowed_rest = (seg_rest[:, None] == seg_rest[None, :])[None]
    features = w_qkv.shape[2]
    heads_local = features // HEAD

    saved = []
    for index in range(2):
        inputs = wide(inputs_pair[index])
        cosine, sine = rotary(position_pair[index])
        allowed = allowed_rest if index == 0 else None
        unit_one, scale_one = norm_parts(inputs)
        normed_one = low(unit_one * attn_gain)
        mixed = jnp.einsum("td,dcf->tcf", normed_one, w_qkv, preferred_element_type=jnp.float32)
        queries = low(spin(mixed[:, 0].reshape(half, heads_local, HEAD), cosine, sine))
        keys = low(spin(mixed[:, 1].reshape(half, heads_local, HEAD), cosine, sine))
        content = low(mixed[:, 2].reshape(half, heads_local, HEAD))
        scores = scores_of(queries, keys, allowed)
        highest = jnp.max(scores, axis=-1, keepdims=True)
        raised = jnp.exp(scores - highest)
        summed = jnp.sum(raised, axis=-1, keepdims=True)
        probs = low(raised / summed)
        attended = low(
            jnp.einsum("hqk,khe->qhe", probs, content, preferred_element_type=jnp.float32)
        ).reshape(half, features)
        branch = jnp.dot(attended, w_out, preferred_element_type=jnp.float32)
        saved.append(
            dict(
                inputs=inputs,
                cosine=cosine,
                sine=sine,
                allowed=allowed,
                normed_one=normed_one,
                queries=queries,
                keys=keys,
                content=content,
                log_total=highest + jnp.log(summed),
                attended=attended,
                branch=branch,
            )
        )
    for index in range(2):
        kept = saved[index]
        kept["hidden"] = kept["inputs"] + swap_sum(kept["branch"])
    for index in range(2):
        kept = saved[index]
        grad_y = grads_pair[index]
        unit_two, scale_two = norm_parts(kept["hidden"])
        normed_two = low(unit_two * mlp_gain)
        gate_up = jnp.einsum("td,dcf->tcf", normed_two, w_in, preferred_element_type=jnp.float32)
        inner, gate = (gate_up[:, 0], gate_up[:, 1])
        below = 0.5 + 0.5 * lax.erf(inner * ROOT_HALF)
        active = inner * below
        slope = below + inner * (ROOT_TWO_PI_INV * jnp.exp(-0.5 * inner * inner))
        product = low(active * gate)
        kept["mlp_part"] = jnp.dot(product, w_down, preferred_element_type=jnp.float32)
        grad_product = jnp.einsum("td,fd->tf", grad_y, w_down, preferred_element_type=jnp.float32)
        grad_inner = low(grad_product * gate * slope)
        grad_gate = low(grad_product * active)
        kept["normed_two_part"] = jnp.einsum(
            "tf,df->td", grad_inner, w_in[:, 0], preferred_element_type=jnp.float32
        ) + jnp.einsum("tf,df->td", grad_gate, w_in[:, 1], preferred_element_type=jnp.float32)
        kept.update(
            normed_two=normed_two, product=product, grad_inner=grad_inner, grad_gate=grad_gate
        )
    for index in range(2):
        kept = saved[index]
        kept["grad_normed_two"] = swap_sum(kept["normed_two_part"])
    for index in range(2):
        kept = saved[index]
        kept["result"] = kept["hidden"] + swap_sum(kept["mlp_part"])

    for index in range(2):
        kept = saved[index]
        unit_two, scale_two = norm_parts(kept["hidden"])
        back = kept["grad_normed_two"]
        kept["mlp_gain_grad"] = jnp.sum(back * unit_two, axis=0)
        grad_hidden = wide(grads_pair[index]) + norm_back(unit_two, scale_two, back * mlp_gain)
        grad_branch = low(grad_hidden)
        upstream = low(
            jnp.einsum("td,fd->tf", grad_branch, w_out, preferred_element_type=jnp.float32)
        ).reshape(half, heads_local, HEAD)
        queries, keys, content = (kept["queries"], kept["keys"], kept["content"])
        probs = jnp.exp(scores_of(queries, keys, kept["allowed"]) - kept["log_total"])
        grad_probs = jnp.einsum(
            "qhe,khe->hqk", upstream, content, preferred_element_type=jnp.float32
        )
        weighted = jnp.sum(probs * grad_probs, axis=-1, keepdims=True)
        grad_scores = low(probs * (grad_probs - weighted))
        query_grad = (
            jnp.einsum("hqk,khe->qhe", grad_scores, keys, preferred_element_type=jnp.float32)
            * SCORE_SCALE
        )
        key_grad = (
            jnp.einsum("hqk,qhe->khe", grad_scores, queries, preferred_element_type=jnp.float32)
            * SCORE_SCALE
        )
        value_grad = jnp.einsum(
            "hqk,qhe->khe", low(probs), upstream, preferred_element_type=jnp.float32
        )
        grad_mixed = jnp.concatenate(
            [
                low(spin_back(query_grad, kept["cosine"], kept["sine"])).reshape(half, features),
                low(spin_back(key_grad, kept["cosine"], kept["sine"])).reshape(half, features),
                low(value_grad).reshape(half, features),
            ],
            axis=1,
        )
        kept["normed_one_part"] = jnp.einsum(
            "tf,df->td",
            grad_mixed,
            w_qkv.reshape(model_width, 3 * features),
            preferred_element_type=jnp.float32,
        )
        kept.update(grad_hidden=grad_hidden, grad_branch=grad_branch, grad_mixed=grad_mixed)
    for index in range(2):
        kept = saved[index]
        back = swap_sum(kept["normed_one_part"])
        unit_one, scale_one = norm_parts(kept["inputs"])
        kept["attn_gain_grad"] = jnp.sum(back * unit_one, axis=0)
        kept["grad_inputs"] = kept["grad_hidden"] + norm_back(unit_one, scale_one, back * attn_gain)

    rest, long = saved

    def send_back(name):
        joined = low(join(rest[name], long[name]))
        home = deal(take_pieces(joined, in_place, piece_count))
        return wide(take_pieces(home, own_slots, slot_count))

    back_y = send_back("result")
    back_dx = send_back("grad_inputs")

    def both(name):
        return jnp.concatenate([rest[name], long[name]], axis=0)

    def weight_grad(left, right):
        grad = lax.dot_general(
            left, right, (((0,), (0,)), ((), ())), preferred_element_type=jnp.float32
        )
        return scatter_sum(grad, group_total, group_index)

    grads_both = jnp.concatenate(grads_pair, axis=0)
    normed_two = both("normed_two")
    shard_down = weight_grad(grads_both, both("product")).T
    shard_inner = weight_grad(normed_two, both("grad_inner"))
    shard_gate = weight_grad(normed_two, both("grad_gate"))
    shard_out = weight_grad(both("grad_branch"), both("attended")).T
    shard_qkv = weight_grad(both("normed_one"), both("grad_mixed"))
    gains = jnp.stack(
        [
            rest["attn_gain_grad"] + long["attn_gain_grad"],
            rest["mlp_gain_grad"] + long["mlp_gain_grad"],
        ]
    )
    gains = lax.psum_scatter(gains, "dp", scatter_dimension=1, tiled=True)
    return (
        back_y,
        back_dx,
        gains[0],
        gains[1],
        shard_qkv.reshape(-1, 3, features),
        shard_out,
        jnp.stack([shard_inner, shard_gate], axis=1),
        shard_down,
    )


def solution(mesh):
    placed = (
        P("dp", None),
        P("dp", None),
        P(),
        P(),
        P(None, None, "tensor"),
        P("tensor", None),
        P(None, None, "tensor"),
        P("tensor", None),
        P(),
        P(),
        P(),
    )
    return jax.shard_map(
        on_device,
        mesh=mesh,
        in_specs=placed,
        out_specs=(
            P("dp", None),
            P("dp", None),
            P("dp"),
            P("dp"),
            P("dp", None, "tensor"),
            P("tensor", "dp"),
            P("dp", None, "tensor"),
            P("tensor", "dp"),
        ),
        check_vma=False,
    )
```

```python
import jax
import jax.numpy as jnp
from jax import lax
from jax.sharding import PartitionSpec as P

HEAD = 64
EPSILON = 1e-05
THETA_BASE = 160000.0
SCORE_SCALE = 0.125
MASK_FILL = -1000000000.0
ROOT_HALF = 0.7071067811865476
ROOT_TWO_PI_INV = 0.3989422804014327


def low(values):
    return values.astype(jnp.bfloat16)


def wide(values):
    return values.astype(jnp.float32)


def norm_parts(values):
    centred = values - jnp.mean(values, axis=-1, keepdims=True)
    scale = lax.rsqrt(jnp.mean(centred * centred, axis=-1, keepdims=True) + EPSILON)
    return (centred * scale, scale)


def norm_back(unit, scale, grad):
    mean_grad = jnp.mean(grad, axis=-1, keepdims=True)
    mean_along = jnp.mean(grad * unit, axis=-1, keepdims=True)
    return scale * (grad - mean_grad - unit * mean_along)


def rotary(position):
    halves = HEAD // 2
    frequency = THETA_BASE ** (-2.0 * jnp.arange(halves, dtype=jnp.float32) / HEAD)
    angles = position.astype(jnp.float32)[:, None] * frequency[None, :]
    cosine = jnp.concatenate([jnp.cos(angles), jnp.cos(angles)], axis=-1)[:, None, :]
    sine = jnp.concatenate([jnp.sin(angles), jnp.sin(angles)], axis=-1)[:, None, :]
    return (cosine, sine)


def spin(values, cosine, sine):
    halves = values.shape[-1] // 2
    turned = jnp.concatenate([-values[..., halves:], values[..., :halves]], axis=-1)
    return values * cosine + turned * sine


def spin_back(grads, cosine, sine):
    halves = grads.shape[-1] // 2
    scaled = grads * sine
    turned = jnp.concatenate([scaled[..., halves:], -scaled[..., :halves]], axis=-1)
    return grads * cosine + turned


def segments(lengths_row, row_count):
    ends = jnp.cumsum(lengths_row)
    rows = jnp.arange(row_count, dtype=jnp.int32)
    segment = jnp.sum((rows[:, None] >= ends[None, :]).astype(jnp.int32), axis=1)
    starts = ends - lengths_row
    matches = segment[:, None] == jnp.arange(lengths_row.shape[0], dtype=jnp.int32)[None, :]
    first_rows = jnp.sum(jnp.where(matches, starts[None, :], 0), axis=1)
    long_start = jnp.sum(jnp.where(lengths_row * 2 == row_count, starts, 0))
    return (segment, rows - first_rows, long_start)


class Swap:
    def __init__(self, part, *earlier):
        self.mine = after(low(part), *earlier)
        self.other = lax.ppermute(self.mine, "tensor", [(0, 1), (1, 0)])

    def total(self, *earlier):
        return wide(self.mine) + wide(after(self.other, *earlier))


class Halving:
    def __init__(self, grad, group_total, group_index, send_type=jnp.bfloat16):
        self.grad = grad
        self.group_total = group_total
        self.group_index = group_index
        self.send_type = send_type
        self.bits = group_total.bit_length() - 1
        self.bit = 0
        rows = grad.shape[0] // group_total
        self.value = grad.reshape((2,) * self.bits + (rows,) + grad.shape[1:])

    def stage(self, *earlier):
        if self.bit == self.bits:
            return self.value
        bit, self.bit = self.bit, self.bit + 1
        axis = self.bits - 1 - bit
        mine = (self.group_index >> bit) & 1
        send = lax.dynamic_index_in_dim(self.value, 1 - mine, axis, keepdims=False)
        keep = lax.dynamic_index_in_dim(self.value, mine, axis, keepdims=False)
        pairs = [(device, device ^ (1 << bit)) for device in range(self.group_total)]
        got = lax.ppermute(send.astype(self.send_type), "dp", pairs)
        self.value = keep + wide(after(got, *earlier))
        return got

    def finish(self):
        while self.bit < self.bits:
            self.stage()
        return self.value


def after(value, *earlier):
    return lax.optimization_barrier((value,) + earlier)[0]


def scores_of(queries, keys, allowed):
    scores = (
        jnp.einsum("qhe,khe->hqk", queries, keys, preferred_element_type=jnp.float32) * SCORE_SCALE
    )
    if allowed is not None:
        scores = jnp.where(allowed, scores, MASK_FILL)
    return scores


def on_device(
    tokens,
    cotangent,
    attn_gain,
    mlp_gain,
    w_qkv,
    w_out,
    w_in,
    w_down,
    seq_lengths,
    set_owner,
    arrival,
):
    group_total = lax.axis_size("dp")
    group_index = lax.axis_index("dp")
    row_count = tokens.shape[0]
    model_width = tokens.shape[1]
    piece_count = arrival.shape[0] // group_total
    piece_rows = row_count // piece_count
    pair_cap = max(2, piece_count // group_total)
    slot_count = group_total * pair_cap
    target = arrival.reshape(group_total, piece_count)
    target_group = target // piece_count
    target_place = target % piece_count
    piece_ids = jnp.arange(piece_count, dtype=jnp.int32)
    earlier = piece_ids[None, :] < piece_ids[:, None]
    same_group = target_group[:, :, None] == target_group[:, None, :]
    slot_rank = jnp.sum((same_group & earlier[None]).astype(jnp.int32), axis=2)
    send_slot = target_group * pair_cap + slot_rank
    own_slots = lax.dynamic_index_in_dim(send_slot, group_index, 0, keepdims=False)
    slot_ids = jnp.arange(slot_count, dtype=jnp.int32)
    outgoing = own_slots[None, :] == slot_ids[:, None]
    out_piece = jnp.sum(jnp.where(outgoing, piece_ids[None, :], 0), axis=1)
    toward = target_group == group_index
    rank_ids = jnp.arange(pair_cap, dtype=jnp.int32)
    incoming = toward[:, None, :] & (slot_rank[:, None, :] == rank_ids[None, :, None])
    in_place = jnp.sum(jnp.where(incoming, target_place[:, None, :], 0), axis=2).reshape(slot_count)
    in_live = jnp.any(incoming, axis=2).reshape(slot_count)
    chosen = (in_place[None, :] == piece_ids[:, None]) & in_live[None, :]
    in_slot = jnp.sum(jnp.where(chosen, slot_ids[None, :], 0), axis=1)

    def take_pieces(values, ids, count):
        return (
            values.reshape(count, piece_rows, model_width)
            .at[ids]
            .get(mode="promise_in_bounds")
            .reshape(-1, model_width)
        )

    def deal(values):
        return lax.all_to_all(values, "dp", split_axis=0, concat_axis=0, tiled=True)

    held = set_owner == group_index
    lengths_mine = jnp.sum(jnp.where(held[:, None], seq_lengths, 0), axis=0)
    segment, position, long_start = segments(lengths_mine, row_count)
    half = row_count // 2
    low_first = jnp.arange(half, dtype=jnp.int32) < long_start

    def split(values):
        mask = low_first.reshape((half,) + (1,) * (values.ndim - 1))
        first, second = (values[:half], values[half:])
        return (jnp.where(mask, first, second), jnp.where(mask, second, first))

    def join(rest, long):
        mask = low_first.reshape((half,) + (1,) * (rest.ndim - 1))
        return jnp.concatenate([jnp.where(mask, rest, long), jnp.where(mask, long, rest)], axis=0)

    tokens_in = deal(take_pieces(tokens, out_piece, piece_count))
    inputs_pair = split(take_pieces(tokens_in, in_slot, slot_count))
    position_pair = split(position)
    seg_rest, _ = split(segment)
    allowed_rest = (seg_rest[:, None] == seg_rest[None, :])[None]
    features = w_qkv.shape[2]
    heads_local = features // HEAD

    saved = []
    for index in range(2):
        inputs = wide(inputs_pair[index])
        cosine, sine = rotary(position_pair[index])
        allowed = allowed_rest if index == 0 else None
        unit_one, scale_one = norm_parts(inputs)
        normed_one = low(unit_one * attn_gain)
        mixed = jnp.einsum("td,dcf->tcf", normed_one, w_qkv, preferred_element_type=jnp.float32)
        queries = low(spin(mixed[:, 0].reshape(half, heads_local, HEAD), cosine, sine))
        keys = low(spin(mixed[:, 1].reshape(half, heads_local, HEAD), cosine, sine))
        content = low(mixed[:, 2].reshape(half, heads_local, HEAD))
        scores = scores_of(queries, keys, allowed)
        highest = jnp.max(scores, axis=-1, keepdims=True)
        raised = jnp.exp(scores - highest)
        summed = jnp.sum(raised, axis=-1, keepdims=True)
        probs = low(raised / summed)
        attended = low(
            jnp.einsum("hqk,khe->qhe", probs, content, preferred_element_type=jnp.float32)
        ).reshape(half, features)
        branch = jnp.dot(attended, w_out, preferred_element_type=jnp.float32)
        saved.append(
            dict(
                inputs=inputs,
                cosine=cosine,
                sine=sine,
                allowed=allowed,
                normed_one=normed_one,
                queries=queries,
                keys=keys,
                content=content,
                log_total=highest + jnp.log(summed),
                attended=attended,
                branch=branch,
            )
        )
        if index == 0:
            packed_grads = after(take_pieces(cotangent, out_piece, piece_count), attended)
            grads_in = deal(packed_grads)
        saved[index]["swap"] = Swap(branch)
    rest, long = saved
    grads_pair = split(take_pieces(grads_in, in_slot, slot_count))
    for index in range(2):
        kept = saved[index]
        grad_y = grads_pair[index]
        if index == 0:
            total = rest["swap"].total(long["swap"].mine)
        else:
            total = long["swap"].total(rest["swap"].mine)
        kept["hidden"] = kept["inputs"] + total
        unit_two, scale_two = norm_parts(kept["hidden"])
        normed_two = low(unit_two * mlp_gain)
        gate_up = jnp.einsum("td,dcf->tcf", normed_two, w_in, preferred_element_type=jnp.float32)
        inner, gate = (gate_up[:, 0], gate_up[:, 1])
        below = 0.5 + 0.5 * lax.erf(inner * ROOT_HALF)
        active = inner * below
        slope = below + inner * (ROOT_TWO_PI_INV * jnp.exp(-0.5 * inner * inner))
        product = low(active * gate)
        grad_product = jnp.einsum("td,fd->tf", grad_y, w_down, preferred_element_type=jnp.float32)
        grad_inner = low(grad_product * gate * slope)
        grad_gate = low(grad_product * active)
        part = jnp.einsum(
            "tf,df->td", grad_inner, w_in[:, 0], preferred_element_type=jnp.float32
        ) + jnp.einsum("tf,df->td", grad_gate, w_in[:, 1], preferred_element_type=jnp.float32)
        kept["swap"] = Swap(part)
        kept.update(
            normed_two=normed_two, product=product, grad_inner=grad_inner, grad_gate=grad_gate
        )

    def both(name):
        return jnp.concatenate([rest[name], long[name]], axis=0)

    def weight_grad(left, right):
        grad = lax.dot_general(
            left, right, (((0,), (0,)), ((), ())), preferred_element_type=jnp.float32
        )
        return Halving(grad, group_total, group_index)

    grads_both = jnp.concatenate(grads_pair, axis=0)
    normed_both = both("normed_two")
    sums_two = [
        weight_grad(grads_both, both("product")),
        weight_grad(normed_both, both("grad_inner")),
        weight_grad(normed_both, both("grad_gate")),
    ]
    for kept in saved:
        mlp_part = jnp.dot(kept["product"], w_down, preferred_element_type=jnp.float32)
        kept["mlp_swap"] = Swap(mlp_part, long["swap"].mine)

    for index in range(2):
        kept = saved[index]
        if index == 0:
            back = kept["swap"].total(
                long["mlp_swap"].mine, long["swap"].mine, *[part.grad for part in sums_two]
            )
        else:
            back = kept["swap"].total(
                rest["last_swap"].mine, *[part.stage() for part in sums_two]
            )
        unit_two, scale_two = norm_parts(kept["hidden"])
        kept["mlp_gain_grad"] = jnp.sum(back * unit_two, axis=0)
        grad_hidden = wide(grads_pair[index]) + norm_back(unit_two, scale_two, back * mlp_gain)
        grad_branch = low(grad_hidden)
        upstream = low(
            jnp.einsum("td,fd->tf", grad_branch, w_out, preferred_element_type=jnp.float32)
        ).reshape(half, heads_local, HEAD)
        queries, keys, content = (kept["queries"], kept["keys"], kept["content"])
        probs = jnp.exp(scores_of(queries, keys, kept["allowed"]) - kept["log_total"])
        grad_probs = jnp.einsum(
            "qhe,khe->hqk", upstream, content, preferred_element_type=jnp.float32
        )
        weighted = jnp.sum(probs * grad_probs, axis=-1, keepdims=True)
        grad_scores = low(probs * (grad_probs - weighted))
        query_grad = (
            jnp.einsum("hqk,khe->qhe", grad_scores, keys, preferred_element_type=jnp.float32)
            * SCORE_SCALE
        )
        key_grad = (
            jnp.einsum("hqk,qhe->khe", grad_scores, queries, preferred_element_type=jnp.float32)
            * SCORE_SCALE
        )
        value_grad = jnp.einsum(
            "hqk,qhe->khe", low(probs), upstream, preferred_element_type=jnp.float32
        )
        grad_mixed = jnp.concatenate(
            [
                low(spin_back(query_grad, kept["cosine"], kept["sine"])).reshape(half, features),
                low(spin_back(key_grad, kept["cosine"], kept["sine"])).reshape(half, features),
                low(value_grad).reshape(half, features),
            ],
            axis=1,
        )
        part = jnp.einsum(
            "tf,df->td",
            grad_mixed,
            w_qkv.reshape(model_width, 3 * features),
            preferred_element_type=jnp.float32,
        )
        kept.update(grad_hidden=grad_hidden, grad_branch=grad_branch, grad_mixed=grad_mixed)
        if index == 0:
            kept["last_swap"] = Swap(part)
        else:
            results = [kept["hidden"] + kept["mlp_swap"].total() for kept in saved]
            packed_y = take_pieces(low(join(*results)), in_place, piece_count)
            long["last_swap"] = Swap(part, packed_y)
            home_y = deal(packed_y)
    stage_two = [part.stage() for part in sums_two]
    normed_both = after(both("normed_one"), *stage_two)
    sum_out = weight_grad(both("grad_branch"), both("attended"))
    sum_qkv = weight_grad(normed_both, both("grad_mixed"))
    for index in range(2):
        kept = saved[index]
        if index == 0:
            back = kept["last_swap"].total(sum_out.grad, sum_qkv.grad)
        else:
            back = kept["last_swap"].total(
                sum_out.stage(), sum_qkv.stage(), *[part.stage() for part in sums_two]
            )
        unit_one, scale_one = norm_parts(kept["inputs"])
        kept["attn_gain_grad"] = jnp.sum(back * unit_one, axis=0)
        kept["grad_inputs"] = kept["grad_hidden"] + norm_back(unit_one, scale_one, back * attn_gain)

    packed_dx = take_pieces(
        low(join(rest["grad_inputs"], long["grad_inputs"])), in_place, piece_count
    )
    home_dx = deal(packed_dx)
    gains = jnp.stack(
        [
            (rest[name] + long[name]).reshape(group_total, -1)
            for name in ("attn_gain_grad", "mlp_gain_grad")
        ],
        axis=1,
    )
    gains = Halving(after(gains, packed_dx), group_total, group_index, jnp.float32)
    gains = gains.finish().reshape(2, -1)
    sum_out.stage(packed_dx)
    sum_qkv.stage(packed_dx)
    shard_down, shard_inner, shard_gate = [part.finish() for part in sums_two]
    back_y = wide(take_pieces(home_y, own_slots, slot_count))
    back_dx = wide(take_pieces(home_dx, own_slots, slot_count))
    return (
        back_y,
        back_dx,
        gains[0],
        gains[1],
        sum_qkv.finish().reshape(-1, 3, features),
        sum_out.finish().T,
        jnp.stack([shard_inner, shard_gate], axis=1),
        shard_down.T,
    )


def solution(mesh):
    placed = (
        P("dp", None),
        P("dp", None),
        P(),
        P(),
        P(None, None, "tensor"),
        P("tensor", None),
        P(None, None, "tensor"),
        P("tensor", None),
        P(),
        P(),
        P(),
    )
    return jax.shard_map(
        on_device,
        mesh=mesh,
        in_specs=placed,
        out_specs=(
            P("dp", None),
            P("dp", None),
            P("dp"),
            P("dp"),
            P("dp", None, "tensor"),
            P("tensor", "dp"),
            P("dp", None, "tensor"),
            P("tensor", "dp"),
        ),
        check_vma=False,
    )
```

```python
import jax
import jax.numpy as jnp
from jax import lax
from jax.sharding import PartitionSpec as P


HEAD = 64
EPSILON = 1e-05
THETA_BASE = 160000.0
SCORE_SCALE = 0.125
MASK_FILL = -1000000000.0
ROOT_HALF = 0.7071067811865476
ROOT_TWO_PI_INV = 0.3989422804014327


def low(values):
    return values.astype(jnp.bfloat16)


def wide(values):
    return values.astype(jnp.float32)


def norm_parts(values):
    centred = values - jnp.mean(values, axis=-1, keepdims=True)
    scale = lax.rsqrt(jnp.mean(centred * centred, axis=-1, keepdims=True) + EPSILON)
    return (centred * scale, scale)


def norm_back(unit, scale, grad):
    mean_grad = jnp.mean(grad, axis=-1, keepdims=True)
    mean_along = jnp.mean(grad * unit, axis=-1, keepdims=True)
    return scale * (grad - mean_grad - unit * mean_along)


def rotary(position):
    halves = HEAD // 2
    frequency = THETA_BASE ** (-2.0 * jnp.arange(halves, dtype=jnp.float32) / HEAD)
    angles = position.astype(jnp.float32)[:, None] * frequency[None, :]
    cosine = jnp.concatenate([jnp.cos(angles), jnp.cos(angles)], axis=-1)[:, None, :]
    sine = jnp.concatenate([jnp.sin(angles), jnp.sin(angles)], axis=-1)[:, None, :]
    return (cosine, sine)


def spin(values, cosine, sine):
    halves = values.shape[-1] // 2
    turned = jnp.concatenate([-values[..., halves:], values[..., :halves]], axis=-1)
    return values * cosine + turned * sine


def spin_back(grads, cosine, sine):
    halves = grads.shape[-1] // 2
    scaled = grads * sine
    turned = jnp.concatenate([scaled[..., halves:], -scaled[..., :halves]], axis=-1)
    return grads * cosine + turned


def segments(lengths_row, row_count):
    ends = jnp.cumsum(lengths_row)
    rows = jnp.arange(row_count, dtype=jnp.int32)
    segment = jnp.sum((rows[:, None] >= ends[None, :]).astype(jnp.int32), axis=1)
    starts = ends - lengths_row
    matches = segment[:, None] == jnp.arange(lengths_row.shape[0], dtype=jnp.int32)[None, :]
    first_rows = jnp.sum(jnp.where(matches, starts[None, :], 0), axis=1)
    long_start = jnp.sum(jnp.where(lengths_row * 2 == row_count, starts, 0))
    return (segment, rows - first_rows, long_start)


class Swap:
    def __init__(self, part, *earlier):
        self.mine = after(low(part), *earlier)
        self.other = lax.ppermute(self.mine, "tensor", [(0, 1), (1, 0)])

    def total(self, *earlier):
        return wide(self.mine) + wide(after(self.other, *earlier))


class Halving:
    def __init__(self, grad, group_total, group_index, send_type=jnp.bfloat16):
        self.group_total = group_total
        self.group_index = group_index
        self.send_type = send_type
        self.bits = group_total.bit_length() - 1
        self.bit = 0
        rows = grad.shape[0] // group_total
        self.value = grad.reshape((2,) * self.bits + (rows,) + grad.shape[1:])
        self.prepare()

    def prepare(self):
        if self.bit < self.bits:
            axis = self.bits - 1 - self.bit
            mine = (self.group_index >> self.bit) & 1
            send = lax.dynamic_index_in_dim(self.value, 1 - mine, axis, keepdims=False)
            self.send = send.astype(self.send_type)
            self.keep = lax.dynamic_index_in_dim(self.value, mine, axis, keepdims=False)

    def stage(self, *earlier):
        if self.bit == self.bits:
            return self.value
        bit, self.bit = self.bit, self.bit + 1
        pairs = [(device, device ^ (1 << bit)) for device in range(self.group_total)]
        got = lax.ppermute(self.send, "dp", pairs)
        self.value = self.keep + wide(after(got, *earlier))
        self.prepare()
        return got

    def finish(self):
        while self.bit < self.bits:
            self.stage()
        return self.value


def after(value, *earlier):
    return lax.optimization_barrier((value,) + earlier)[0]


def scores_of(queries, keys, allowed):
    scores = (
        jnp.einsum("qhe,khe->hqk", queries, keys, preferred_element_type=jnp.float32) * SCORE_SCALE
    )
    if allowed is not None:
        scores = jnp.where(allowed, scores, MASK_FILL)
    return scores


def on_device(
    tokens,
    cotangent,
    attn_gain,
    mlp_gain,
    w_qkv,
    w_out,
    w_in,
    w_down,
    seq_lengths,
    set_owner,
    arrival,
):
    group_total = lax.axis_size("dp")
    group_index = lax.axis_index("dp")
    row_count = tokens.shape[0]
    model_width = tokens.shape[1]
    piece_count = arrival.shape[0] // group_total
    piece_rows = row_count // piece_count
    pair_cap = max(2, piece_count // group_total)
    slot_count = group_total * pair_cap
    target = arrival.reshape(group_total, piece_count)
    target_group = target // piece_count
    target_place = target % piece_count
    piece_ids = jnp.arange(piece_count, dtype=jnp.int32)
    earlier = piece_ids[None, :] < piece_ids[:, None]
    same_group = target_group[:, :, None] == target_group[:, None, :]
    slot_rank = jnp.sum((same_group & earlier[None]).astype(jnp.int32), axis=2)
    send_slot = target_group * pair_cap + slot_rank
    own_slots = lax.dynamic_index_in_dim(send_slot, group_index, 0, keepdims=False)
    slot_ids = jnp.arange(slot_count, dtype=jnp.int32)
    outgoing = own_slots[None, :] == slot_ids[:, None]
    out_piece = jnp.sum(jnp.where(outgoing, piece_ids[None, :], 0), axis=1)
    toward = target_group == group_index
    rank_ids = jnp.arange(pair_cap, dtype=jnp.int32)
    incoming = toward[:, None, :] & (slot_rank[:, None, :] == rank_ids[None, :, None])
    in_place = jnp.sum(jnp.where(incoming, target_place[:, None, :], 0), axis=2).reshape(slot_count)
    in_live = jnp.any(incoming, axis=2).reshape(slot_count)
    chosen = (in_place[None, :] == piece_ids[:, None]) & in_live[None, :]
    in_slot = jnp.sum(jnp.where(chosen, slot_ids[None, :], 0), axis=1)

    def take_pieces(values, ids, count):
        return (
            values.reshape(count, piece_rows, model_width)
            .at[ids]
            .get(mode="promise_in_bounds")
            .reshape(-1, model_width)
        )

    def deal(values):
        return lax.all_to_all(values, "dp", split_axis=0, concat_axis=0, tiled=True)

    held = set_owner == group_index
    lengths_mine = jnp.sum(jnp.where(held[:, None], seq_lengths, 0), axis=0)
    segment, position, long_start = segments(lengths_mine, row_count)
    half = row_count // 2
    low_first = jnp.arange(half, dtype=jnp.int32) < long_start

    def split(values):
        mask = low_first.reshape((half,) + (1,) * (values.ndim - 1))
        first, second = (values[:half], values[half:])
        return (jnp.where(mask, first, second), jnp.where(mask, second, first))

    def join(rest, long):
        mask = low_first.reshape((half,) + (1,) * (rest.ndim - 1))
        return jnp.concatenate([jnp.where(mask, rest, long), jnp.where(mask, long, rest)], axis=0)

    tokens_in = deal(take_pieces(tokens, out_piece, piece_count))
    inputs_pair = split(take_pieces(tokens_in, in_slot, slot_count))
    position_pair = split(position)
    seg_rest, _ = split(segment)
    allowed_rest = (seg_rest[:, None] == seg_rest[None, :])[None]
    features = w_qkv.shape[2]
    heads_local = features // HEAD

    saved = []
    for index in range(2):
        inputs = wide(inputs_pair[index])
        cosine, sine = rotary(position_pair[index])
        allowed = allowed_rest if index == 0 else None
        unit_one, scale_one = norm_parts(inputs)
        normed_one = low(unit_one * attn_gain)
        mixed = jnp.einsum("td,dcf->tcf", normed_one, w_qkv, preferred_element_type=jnp.float32)
        queries = low(spin(mixed[:, 0].reshape(half, heads_local, HEAD), cosine, sine))
        keys = low(spin(mixed[:, 1].reshape(half, heads_local, HEAD), cosine, sine))
        content = low(mixed[:, 2].reshape(half, heads_local, HEAD))
        scores = scores_of(queries, keys, allowed)
        highest = jnp.max(scores, axis=-1, keepdims=True)
        raised = jnp.exp(scores - highest)
        summed = jnp.sum(raised, axis=-1, keepdims=True)
        probs = low(raised / summed)
        attended = low(
            jnp.einsum("hqk,khe->qhe", probs, content, preferred_element_type=jnp.float32)
        ).reshape(half, features)
        branch = jnp.dot(attended, w_out, preferred_element_type=jnp.float32)
        saved.append(
            dict(
                inputs=inputs,
                cosine=cosine,
                sine=sine,
                allowed=allowed,
                normed_one=normed_one,
                queries=queries,
                keys=keys,
                content=content,
                log_total=highest + jnp.log(summed),
                attended=attended,
                branch=branch,
            )
        )
        saved[index]["swap"] = Swap(branch)
    rest, long = saved
    grads_in = deal(take_pieces(cotangent, out_piece, piece_count))
    grads_in = after(grads_in, long["swap"].mine)
    grads_pair = split(take_pieces(grads_in, in_slot, slot_count))
    for index in range(2):
        kept = saved[index]
        grad_y = grads_pair[index]
        if index == 0:
            total = rest["swap"].total(long["swap"].mine)
        else:
            total = long["swap"].total(rest["swap"].mine)
        kept["hidden"] = kept["inputs"] + total
        unit_two, scale_two = norm_parts(kept["hidden"])
        normed_two = low(unit_two * mlp_gain)
        gate_up = jnp.einsum("td,dcf->tcf", normed_two, w_in, preferred_element_type=jnp.float32)
        inner, gate = (gate_up[:, 0], gate_up[:, 1])
        below = 0.5 + 0.5 * lax.erf(inner * ROOT_HALF)
        active = inner * below
        slope = below + inner * (ROOT_TWO_PI_INV * jnp.exp(-0.5 * inner * inner))
        product = low(active * gate)
        grad_product = jnp.einsum("td,fd->tf", grad_y, w_down, preferred_element_type=jnp.float32)
        grad_inner = low(grad_product * gate * slope)
        grad_gate = low(grad_product * active)
        part = jnp.einsum(
            "tf,df->td", grad_inner, w_in[:, 0], preferred_element_type=jnp.float32
        ) + jnp.einsum("tf,df->td", grad_gate, w_in[:, 1], preferred_element_type=jnp.float32)
        kept["swap"] = Swap(part)
        kept.update(
            normed_two=normed_two, product=product, grad_inner=grad_inner, grad_gate=grad_gate
        )

    def both(name):
        return jnp.concatenate([rest[name], long[name]], axis=0)

    def weight_grad(left, right):
        grad = lax.dot_general(
            left, right, (((0,), (0,)), ((), ())), preferred_element_type=jnp.float32
        )
        return Halving(grad, group_total, group_index)

    grads_both = jnp.concatenate(grads_pair, axis=0)
    grads_both, normed_both = lax.optimization_barrier(
        (grads_both, both("normed_two"), long["swap"].mine)
    )[:2]
    sums_two = [
        weight_grad(grads_both, both("product")),
        weight_grad(normed_both, both("grad_inner")),
        weight_grad(normed_both, both("grad_gate")),
    ]
    for kept in saved:
        product = after(kept["product"], long["swap"].mine)
        mlp_part = jnp.dot(product, w_down, preferred_element_type=jnp.float32)
        kept["mlp_swap"] = Swap(mlp_part, rest["swap"].other)

    for index in range(2):
        kept = saved[index]
        if index == 0:
            back = kept["swap"].total(
                long["swap"].mine, *[part.send for part in sums_two]
            )
        else:
            back = kept["swap"].total(
                rest["last_swap"].mine, *[part.stage() for part in sums_two]
            )
        unit_two, scale_two = norm_parts(kept["hidden"])
        kept["mlp_gain_grad"] = jnp.sum(back * unit_two, axis=0)
        grad_hidden = wide(grads_pair[index]) + norm_back(unit_two, scale_two, back * mlp_gain)
        grad_branch = low(grad_hidden)
        upstream = low(
            jnp.einsum("td,fd->tf", grad_branch, w_out, preferred_element_type=jnp.float32)
        ).reshape(half, heads_local, HEAD)
        queries, keys, content = (kept["queries"], kept["keys"], kept["content"])
        if index == 1:
            results = [half_rows["hidden"] + half_rows["mlp_swap"].total() for half_rows in saved]
            packed_y = take_pieces(low(join(*results)), in_place, piece_count)
            content = after(content, packed_y)
            home_y = deal(packed_y)
        probs = jnp.exp(scores_of(queries, keys, kept["allowed"]) - kept["log_total"])
        grad_probs = jnp.einsum(
            "qhe,khe->hqk", upstream, content, preferred_element_type=jnp.float32
        )
        weighted = jnp.sum(probs * grad_probs, axis=-1, keepdims=True)
        grad_scores = low(probs * (grad_probs - weighted))
        query_grad = (
            jnp.einsum("hqk,khe->qhe", grad_scores, keys, preferred_element_type=jnp.float32)
            * SCORE_SCALE
        )
        key_grad = (
            jnp.einsum("hqk,qhe->khe", grad_scores, queries, preferred_element_type=jnp.float32)
            * SCORE_SCALE
        )
        value_grad = jnp.einsum(
            "hqk,qhe->khe", low(probs), upstream, preferred_element_type=jnp.float32
        )
        grad_mixed = jnp.concatenate(
            [
                low(spin_back(query_grad, kept["cosine"], kept["sine"])).reshape(half, features),
                low(spin_back(key_grad, kept["cosine"], kept["sine"])).reshape(half, features),
                low(value_grad).reshape(half, features),
            ],
            axis=1,
        )
        part = jnp.einsum(
            "tf,df->td",
            grad_mixed,
            w_qkv.reshape(model_width, 3 * features),
            preferred_element_type=jnp.float32,
        )
        kept.update(grad_hidden=grad_hidden, grad_branch=grad_branch, grad_mixed=grad_mixed)
        kept["last_swap"] = Swap(part)
    normed_both = both("normed_one")
    sum_out = weight_grad(both("grad_branch"), both("attended"))
    sum_qkv = weight_grad(normed_both, both("grad_mixed"))
    for index in range(2):
        kept = saved[index]
        if index == 0:
            back = kept["last_swap"].total(sum_out.send, sum_qkv.send)
        else:
            back = kept["last_swap"].total(
                home_y,
                *[part.stage(long["last_swap"].mine) for part in sums_two + [sum_out, sum_qkv]],
            )
        unit_one, scale_one = norm_parts(kept["inputs"])
        kept["attn_gain_grad"] = jnp.sum(back * unit_one, axis=0)
        kept["grad_inputs"] = kept["grad_hidden"] + norm_back(unit_one, scale_one, back * attn_gain)

    packed_dx = take_pieces(
        low(join(rest["grad_inputs"], long["grad_inputs"])), in_place, piece_count
    )
    home_dx = deal(packed_dx)
    gains = jnp.stack(
        [
            (rest[name] + long[name]).reshape(group_total, -1)
            for name in ("attn_gain_grad", "mlp_gain_grad")
        ],
        axis=1,
    )
    gains = Halving(after(gains, packed_dx), group_total, group_index, jnp.float32)
    gains = gains.finish().reshape(2, -1)
    for part in (sum_out, sum_qkv):
        part.finish()
    for part in sums_two:
        part.stage()
        part.finish()
    shard_down, shard_inner, shard_gate = [part.value for part in sums_two]
    back_y = wide(take_pieces(home_y, own_slots, slot_count))
    back_dx = wide(take_pieces(after(home_dx, back_y), own_slots, slot_count))
    return (
        back_y,
        back_dx,
        gains[0],
        gains[1],
        sum_qkv.finish().reshape(-1, 3, features),
        sum_out.finish().T,
        jnp.stack([shard_inner, shard_gate], axis=1),
        shard_down.T,
    )


def solution(mesh):
    placed = (
        P("dp", None),
        P("dp", None),
        P(),
        P(),
        P(None, None, "tensor"),
        P("tensor", None),
        P(None, None, "tensor"),
        P("tensor", None),
        P(),
        P(),
        P(),
    )

    return jax.shard_map(
        on_device,
        mesh=mesh,
        in_specs=placed,
        out_specs=(
            P("dp", None),
            P("dp", None),
            P("dp"),
            P("dp"),
            P("dp", None, "tensor"),
            P("tensor", "dp"),
            P("dp", None, "tensor"),
            P("tensor", "dp"),
        ),
        check_vma=False,
    )
```

```python
import jax
import jax.numpy as jnp
from jax import lax
from jax.sharding import PartitionSpec as P


HEAD = 64
EPSILON = 1e-05
THETA_BASE = 160000.0
SCORE_SCALE = 0.125
MASK_FILL = -1000000000.0
ROOT_HALF = 0.7071067811865476
ROOT_TWO_PI_INV = 0.3989422804014327


def low(values):
    return values.astype(jnp.bfloat16)


def wide(values):
    return values.astype(jnp.float32)


def norm_parts(values):
    centred = values - jnp.mean(values, axis=-1, keepdims=True)
    scale = lax.rsqrt(jnp.mean(centred * centred, axis=-1, keepdims=True) + EPSILON)
    return (centred * scale, scale)


def norm_back(unit, scale, grad):
    mean_grad = jnp.mean(grad, axis=-1, keepdims=True)
    mean_along = jnp.mean(grad * unit, axis=-1, keepdims=True)
    return scale * (grad - mean_grad - unit * mean_along)


def rotary(position):
    halves = HEAD // 2
    frequency = THETA_BASE ** (-2.0 * jnp.arange(halves, dtype=jnp.float32) / HEAD)
    angles = position.astype(jnp.float32)[:, None] * frequency[None, :]
    cosine = jnp.concatenate([jnp.cos(angles), jnp.cos(angles)], axis=-1)[:, None, :]
    sine = jnp.concatenate([jnp.sin(angles), jnp.sin(angles)], axis=-1)[:, None, :]
    return (cosine, sine)


def spin(values, cosine, sine):
    halves = values.shape[-1] // 2
    turned = jnp.concatenate([-values[..., halves:], values[..., :halves]], axis=-1)
    return values * cosine + turned * sine


def spin_back(grads, cosine, sine):
    halves = grads.shape[-1] // 2
    scaled = grads * sine
    turned = jnp.concatenate([scaled[..., halves:], -scaled[..., :halves]], axis=-1)
    return grads * cosine + turned


def segments(lengths_row, row_count):
    ends = jnp.cumsum(lengths_row)
    rows = jnp.arange(row_count, dtype=jnp.int32)
    segment = jnp.sum((rows[:, None] >= ends[None, :]).astype(jnp.int32), axis=1)
    starts = ends - lengths_row
    matches = segment[:, None] == jnp.arange(lengths_row.shape[0], dtype=jnp.int32)[None, :]
    first_rows = jnp.sum(jnp.where(matches, starts[None, :], 0), axis=1)
    long_start = jnp.sum(jnp.where(lengths_row * 2 == row_count, starts, 0))
    return (segment, rows - first_rows, long_start)


class Swap:
    def __init__(self, part, *earlier):
        self.mine = after(low(part), *earlier)
        self.other = lax.ppermute(self.mine, "tensor", [(0, 1), (1, 0)])

    def total(self, *earlier):
        return wide(self.mine) + wide(after(self.other, *earlier))


class Halving:
    def __init__(self, grad, group_total, group_index, send_type=jnp.bfloat16):
        self.group_total = group_total
        self.group_index = group_index
        self.send_type = send_type
        self.bits = group_total.bit_length() - 1
        self.bit = 0
        rows = grad.shape[0] // group_total
        self.value = grad.reshape((2,) * self.bits + (rows,) + grad.shape[1:])
        self.prepare()

    def prepare(self):
        if self.bit < self.bits:
            axis = self.bits - 1 - self.bit
            mine = (self.group_index >> self.bit) & 1
            send = lax.dynamic_index_in_dim(self.value, 1 - mine, axis, keepdims=False)
            self.send = send.astype(self.send_type)
            self.keep = lax.dynamic_index_in_dim(self.value, mine, axis, keepdims=False)

    def stage(self, *earlier):
        if self.bit == self.bits:
            return self.value
        bit, self.bit = self.bit, self.bit + 1
        pairs = [(device, device ^ (1 << bit)) for device in range(self.group_total)]
        got = lax.ppermute(self.send, "dp", pairs)
        self.value = self.keep + wide(after(got, *earlier))
        self.prepare()
        return got

    def finish(self):
        while self.bit < self.bits:
            self.stage()
        return self.value


def after(value, *earlier):
    return lax.optimization_barrier((value,) + earlier)[0]


def scores_of(queries, keys, allowed):
    scores = (
        jnp.einsum("qhe,khe->hqk", queries, keys, preferred_element_type=jnp.float32) * SCORE_SCALE
    )
    if allowed is not None:
        scores = jnp.where(allowed, scores, MASK_FILL)
    return scores


def on_device(
    tokens,
    cotangent,
    attn_gain,
    mlp_gain,
    w_qkv,
    w_out,
    w_in,
    w_down,
    seq_lengths,
    set_owner,
    arrival,
):
    group_total = lax.axis_size("dp")
    group_index = lax.axis_index("dp")
    row_count = tokens.shape[0]
    model_width = tokens.shape[1]
    piece_count = arrival.shape[0] // group_total
    piece_rows = row_count // piece_count
    pair_cap = max(2, piece_count // group_total)
    slot_count = group_total * pair_cap
    target = arrival.reshape(group_total, piece_count)
    target_group = target // piece_count
    target_place = target % piece_count
    piece_ids = jnp.arange(piece_count, dtype=jnp.int32)
    earlier = piece_ids[None, :] < piece_ids[:, None]
    same_group = target_group[:, :, None] == target_group[:, None, :]
    slot_rank = jnp.sum((same_group & earlier[None]).astype(jnp.int32), axis=2)
    send_slot = target_group * pair_cap + slot_rank
    own_slots = lax.dynamic_index_in_dim(send_slot, group_index, 0, keepdims=False)
    slot_ids = jnp.arange(slot_count, dtype=jnp.int32)
    outgoing = own_slots[None, :] == slot_ids[:, None]
    out_piece = jnp.sum(jnp.where(outgoing, piece_ids[None, :], 0), axis=1)
    toward = target_group == group_index
    rank_ids = jnp.arange(pair_cap, dtype=jnp.int32)
    incoming = toward[:, None, :] & (slot_rank[:, None, :] == rank_ids[None, :, None])
    in_place = jnp.sum(jnp.where(incoming, target_place[:, None, :], 0), axis=2).reshape(slot_count)
    in_live = jnp.any(incoming, axis=2).reshape(slot_count)
    chosen = (in_place[None, :] == piece_ids[:, None]) & in_live[None, :]
    in_slot = jnp.sum(jnp.where(chosen, slot_ids[None, :], 0), axis=1)

    def take_pieces(values, ids, count):
        return (
            values.reshape(count, piece_rows, model_width)
            .at[ids]
            .get(mode="promise_in_bounds")
            .reshape(-1, model_width)
        )

    def deal(values):
        return lax.all_to_all(values, "dp", split_axis=0, concat_axis=0, tiled=True)

    held = set_owner == group_index
    lengths_mine = jnp.sum(jnp.where(held[:, None], seq_lengths, 0), axis=0)
    segment, position, long_start = segments(lengths_mine, row_count)
    half = row_count // 2
    low_first = jnp.arange(half, dtype=jnp.int32) < long_start

    def split(values):
        mask = low_first.reshape((half,) + (1,) * (values.ndim - 1))
        first, second = (values[:half], values[half:])
        return (jnp.where(mask, first, second), jnp.where(mask, second, first))

    def join(rest, long):
        mask = low_first.reshape((half,) + (1,) * (rest.ndim - 1))
        return jnp.concatenate([jnp.where(mask, rest, long), jnp.where(mask, long, rest)], axis=0)

    tokens_in = deal(take_pieces(tokens, out_piece, piece_count))
    inputs_pair = split(take_pieces(tokens_in, in_slot, slot_count))
    position_pair = split(position)
    seg_rest, _ = split(segment)
    allowed_rest = (seg_rest[:, None] == seg_rest[None, :])[None]
    features = w_qkv.shape[2]
    heads_local = features // HEAD

    saved = []
    for index in range(2):
        inputs = wide(inputs_pair[index])
        cosine, sine = rotary(position_pair[index])
        allowed = allowed_rest if index == 0 else None
        unit_one, scale_one = norm_parts(inputs)
        normed_one = low(unit_one * attn_gain)
        mixed = jnp.einsum("td,dcf->tcf", normed_one, w_qkv, preferred_element_type=jnp.float32)
        queries = low(spin(mixed[:, 0].reshape(half, heads_local, HEAD), cosine, sine))
        keys = low(spin(mixed[:, 1].reshape(half, heads_local, HEAD), cosine, sine))
        content = low(mixed[:, 2].reshape(half, heads_local, HEAD))
        scores = scores_of(queries, keys, allowed)
        highest = jnp.max(scores, axis=-1, keepdims=True)
        raised = jnp.exp(scores - highest)
        summed = jnp.sum(raised, axis=-1, keepdims=True)
        probs = low(raised / summed)
        attended = low(
            jnp.einsum("hqk,khe->qhe", probs, content, preferred_element_type=jnp.float32)
        ).reshape(half, features)
        branch = jnp.dot(attended, w_out, preferred_element_type=jnp.float32)
        saved.append(
            dict(
                inputs=inputs,
                cosine=cosine,
                sine=sine,
                allowed=allowed,
                normed_one=normed_one,
                queries=queries,
                keys=keys,
                content=content,
                log_total=highest + jnp.log(summed),
                attended=attended,
                branch=branch,
            )
        )
        saved[index]["swap"] = Swap(branch)
    rest, long = saved
    grads_in = deal(take_pieces(cotangent, out_piece, piece_count))
    grads_in = after(grads_in, long["swap"].mine)
    grads_pair = split(take_pieces(grads_in, in_slot, slot_count))
    for index in range(2):
        kept = saved[index]
        grad_y = grads_pair[index]
        if index == 0:
            total = rest["swap"].total(long["swap"].mine)
        else:
            total = long["swap"].total(rest["swap"].mine)
        kept["hidden"] = kept["inputs"] + total
        unit_two, scale_two = norm_parts(kept["hidden"])
        normed_two = low(unit_two * mlp_gain)
        gate_up = jnp.einsum("td,dcf->tcf", normed_two, w_in, preferred_element_type=jnp.float32)
        inner, gate = (gate_up[:, 0], gate_up[:, 1])
        below = 0.5 + 0.5 * lax.erf(inner * ROOT_HALF)
        active = inner * below
        slope = below + inner * (ROOT_TWO_PI_INV * jnp.exp(-0.5 * inner * inner))
        product = low(active * gate)
        grad_product = jnp.einsum("td,fd->tf", grad_y, w_down, preferred_element_type=jnp.float32)
        grad_inner = low(grad_product * gate * slope)
        grad_gate = low(grad_product * active)
        part = jnp.einsum(
            "tf,df->td", grad_inner, w_in[:, 0], preferred_element_type=jnp.float32
        ) + jnp.einsum("tf,df->td", grad_gate, w_in[:, 1], preferred_element_type=jnp.float32)
        kept["swap"] = Swap(part)
        kept.update(
            normed_two=normed_two, product=product, grad_inner=grad_inner, grad_gate=grad_gate
        )

    def both(name):
        return jnp.concatenate([rest[name], long[name]], axis=0)

    def weight_grad(left, right):
        grad = lax.dot_general(
            left, right, (((0,), (0,)), ((), ())), preferred_element_type=jnp.float32
        )
        return Halving(grad, group_total, group_index)

    grads_both = jnp.concatenate(grads_pair, axis=0)
    grads_both, normed_both = lax.optimization_barrier(
        (grads_both, both("normed_two"), long["swap"].mine)
    )[:2]
    sums_two = [
        weight_grad(grads_both, both("product")),
        weight_grad(normed_both, both("grad_inner")),
        weight_grad(normed_both, both("grad_gate")),
    ]
    for kept in saved:
        product = after(kept["product"], long["swap"].mine)
        mlp_part = jnp.dot(product, w_down, preferred_element_type=jnp.float32)
        kept["mlp_swap"] = Swap(mlp_part, rest["swap"].other)

    for index in range(2):
        kept = saved[index]
        if index == 0:
            back = kept["swap"].total(
                long["swap"].mine, *[part.send for part in sums_two]
            )
        else:
            back = kept["swap"].total(
                rest["last_swap"].mine, *[part.stage() for part in sums_two]
            )
        unit_two, scale_two = norm_parts(kept["hidden"])
        kept["mlp_gain_grad"] = jnp.sum(back * unit_two, axis=0)
        grad_hidden = wide(grads_pair[index]) + norm_back(unit_two, scale_two, back * mlp_gain)
        grad_branch = low(grad_hidden)
        upstream = low(
            jnp.einsum("td,fd->tf", grad_branch, w_out, preferred_element_type=jnp.float32)
        ).reshape(half, heads_local, HEAD)
        queries, keys, content = (kept["queries"], kept["keys"], kept["content"])
        if index == 1:
            results = [half_rows["hidden"] + half_rows["mlp_swap"].total() for half_rows in saved]
            packed_y = take_pieces(low(join(*results)), in_place, piece_count)
            content = after(content, packed_y)
            home_y = deal(packed_y)
        probs = jnp.exp(scores_of(queries, keys, kept["allowed"]) - kept["log_total"])
        grad_probs = jnp.einsum(
            "qhe,khe->hqk", upstream, content, preferred_element_type=jnp.float32
        )
        weighted = jnp.sum(probs * grad_probs, axis=-1, keepdims=True)
        grad_scores = low(probs * (grad_probs - weighted))
        query_grad = (
            jnp.einsum("hqk,khe->qhe", grad_scores, keys, preferred_element_type=jnp.float32)
            * SCORE_SCALE
        )
        key_grad = (
            jnp.einsum("hqk,qhe->khe", grad_scores, queries, preferred_element_type=jnp.float32)
            * SCORE_SCALE
        )
        value_grad = jnp.einsum(
            "hqk,qhe->khe", low(probs), upstream, preferred_element_type=jnp.float32
        )
        grad_mixed = jnp.concatenate(
            [
                low(spin_back(query_grad, kept["cosine"], kept["sine"])).reshape(half, features),
                low(spin_back(key_grad, kept["cosine"], kept["sine"])).reshape(half, features),
                low(value_grad).reshape(half, features),
            ],
            axis=1,
        )
        part = jnp.einsum(
            "tf,df->td",
            grad_mixed,
            w_qkv.reshape(model_width, 3 * features),
            preferred_element_type=jnp.float32,
        )
        kept.update(grad_hidden=grad_hidden, grad_branch=grad_branch, grad_mixed=grad_mixed)
        kept["last_swap"] = Swap(part)
    normed_both = both("normed_one")
    sum_out = weight_grad(both("grad_branch"), both("attended"))
    sum_qkv = weight_grad(normed_both, both("grad_mixed"))
    for index in range(2):
        kept = saved[index]
        if index == 0:
            back = kept["last_swap"].total(sum_out.send, sum_qkv.send)
        else:
            back = kept["last_swap"].total(
                home_y,
                *[part.stage(long["last_swap"].mine) for part in sums_two + [sum_out, sum_qkv]],
            )
        unit_one, scale_one = norm_parts(kept["inputs"])
        kept["attn_gain_grad"] = jnp.sum(back * unit_one, axis=0)
        kept["grad_inputs"] = kept["grad_hidden"] + norm_back(unit_one, scale_one, back * attn_gain)

    packed_dx = take_pieces(
        low(join(rest["grad_inputs"], long["grad_inputs"])), in_place, piece_count
    )
    home_dx = deal(packed_dx)
    gains = jnp.stack(
        [
            (rest[name] + long[name]).reshape(group_total, -1)
            for name in ("attn_gain_grad", "mlp_gain_grad")
        ],
        axis=1,
    )
    gains = Halving(after(gains, packed_dx), group_total, group_index, jnp.float32)
    gains = gains.finish().reshape(2, -1)
    back_y = wide(take_pieces(home_y, own_slots, slot_count))
    back_dx = wide(take_pieces(after(home_dx, back_y), own_slots, slot_count))
    while sum_qkv.bit < sum_qkv.bits:
        sum_out.stage()
        sum_qkv.stage(*([back_dx] if sum_qkv.bit == sum_qkv.bits - 2 else []))
    for part in sums_two:
        part.stage()
        part.finish()
    shard_down, shard_inner, shard_gate = [part.value for part in sums_two]
    return (
        back_y,
        back_dx,
        gains[0],
        gains[1],
        sum_qkv.finish().reshape(-1, 3, features),
        sum_out.finish().T,
        jnp.stack([shard_inner, shard_gate], axis=1),
        shard_down.T,
    )


def solution(mesh):
    placed = (
        P("dp", None),
        P("dp", None),
        P(),
        P(),
        P(None, None, "tensor"),
        P("tensor", None),
        P(None, None, "tensor"),
        P("tensor", None),
        P(),
        P(),
        P(),
    )

    return jax.shard_map(
        on_device,
        mesh=mesh,
        in_specs=placed,
        out_specs=(
            P("dp", None),
            P("dp", None),
            P("dp"),
            P("dp"),
            P("dp", None, "tensor"),
            P("tensor", "dp"),
            P("dp", None, "tensor"),
            P("tensor", "dp"),
        ),
        check_vma=False,
    )
```
